256 devices in a mesh: groups: 2 (over z), rows: 64 (over y, x), cols: 2 (over core).
Axes of the slice: x: 8, y: 8, z: 2, core: 2. Of those that a mesh axis runs over, the one named last changes fastest.
The devices are a block of a 8x8x16 slice.
Arguments:
- feature_table: float32 [262144, 1024], P(('groups', 'rows'), 'cols'), parts along dimension 0, may hold values from -6 to 6
- own_features: float32 [4096, 1024], P(('groups', 'rows'), 'cols'), parts along dimension 0, may hold values from -6 to 6
- neighbor_ids: int32 [4096, 50], P(('groups', 'rows')), parts along dimension 0, may hold values from 0 to 131071, as said below
- importance: float32 [4096, 50], P(('groups', 'rows')), parts along dimension 0, may hold values from 0.5 to 5
- w_self: bfloat16 [1024, 1024], P('cols'), may hold values from -0.1875 to 0.1875
- w_pool: bfloat16 [1024, 1024], P('cols'), may hold values from -0.1875 to 0.1875
- bias: float32 [1024], replicated, may hold values from -6 to 6
Outputs:
- embeddings: float32 [4096, 1024], P(('groups', 'rows'), 'cols'), parts along dimension 0
The draws below stay inside these ranges and needn't reach their ends.
There are 2 independent parts, one for each index of `groups`. The reference program is written for one: setup_inputs(seed, part) draws one part's arguments, and reference() takes and returns one part's arrays. A program takes and returns all parts, laid end to end along the dimension named above; an argument that names none is the same for every part. Nothing has to cross between parts.
Inputs may be any that keep to these rules, and one draw needn't show every extreme that they name: `neighbor_ids`: ids of sampled neighbors in the group's table, repeats allowed. In each aligned block of 16 targets, at most 20 ids fall in any one range [k * 2048, (k + 1) * 2048), and one such range holds exactly 20.
All inputs are finite; a program needn't handle non-finite values.
Results may differ from the reference program's by a relative error of at most 0.0017.
Values may be sent and summed in bfloat16 or wider, within the bound.
A program may use at most 64 MiB of HBM per device.

```python
import math
import jax
import jax.numpy as jnp
from jax import lax

D = 1024
NEIGH = 50
TGT_DEV = 16
ROWS_DEV = 2048
CAP = 20
TARGETS = 2048
NODES = 131072


def draw_device(key_device):
    owners = NODES // ROWS_DEV
    per_device = TARGETS // (TGT_DEV * owners)
    slot_count = owners * CAP
    requests = TGT_DEV * NEIGH
    key_busy, key_owner, key_blocks = jax.random.split(key_device, 3)
    slot_index = jnp.arange(slot_count, dtype=jnp.int32)
    labels = slot_index // CAP
    within = slot_index - labels * CAP
    busiest = jax.random.randint(key_busy, (), 0, owners, dtype=jnp.int32)
    owner_order = jax.random.permutation(key_owner, owners).astype(jnp.int32)
    owner_rank = jnp.argsort(owner_order, stable=True).astype(jnp.int32)
    category = jnp.where(labels == busiest, 0, jnp.where(within < CAP - 1, 1, 2)).astype(jnp.int32)
    scores = category * slot_count + owner_rank[labels] * CAP + within
    ordering = jnp.argsort(scores, stable=True)
    chosen = labels[ordering[:requests]]
    block_keys = jax.random.split(key_blocks, per_device)

    def one_block(key_block):
        key_order, key_local = jax.random.split(key_block, 2)
        picked = jax.random.permutation(key_order, chosen)
        local_row = jax.random.randint(key_local, (requests,), 0, ROWS_DEV, dtype=jnp.int32)
        return (picked * ROWS_DEV + local_row).reshape(TGT_DEV, NEIGH)
    return jax.vmap(one_block)(block_keys)


def draw_neighbor_ids(key, part):
    owners = NODES // ROWS_DEV
    keys_all = jax.random.split(jax.random.fold_in(key, 11), owners)
    return jax.vmap(draw_device)(keys_all).reshape(TARGETS, NEIGH)


def draw_bias(key, part):
    column_scale = 0.3 + 1.7 * jnp.arange(D, dtype=jnp.float32) / D
    values = jax.random.normal(jax.random.fold_in(key, 5), (D,), jnp.float32) * column_scale
    return jnp.clip(values, -6.0, 6.0)


def levels(own_key, shape, shards, smallest, top_value):
    gain = 1.0
    for axis_at, parts in shards:
        steps = jax.random.uniform(jax.random.fold_in(jax.random.fold_in(own_key, 6), axis_at), (parts,), jnp.float32, smallest / len(shards), top_value / len(shards))
        gain = gain * jnp.repeat(jnp.exp(steps), shape[axis_at] // parts).reshape((-1,) + (1,) * (len(shape) - 1 - axis_at))
    return gain


def centred(rng, extent, scale, limit, cuts=(), held_as=jnp.bfloat16):
    result = jax.random.normal(rng, extent, jnp.float32) * scale
    if len(cuts) > 0:
        result = levels(rng, extent, cuts, -0.22, 0.18) * result
    return jnp.clip(result, min=-limit, max=limit).astype(held_as)


def setup_inputs(seed: int = 0, part: int = 0) -> dict:
    keys = jax.random.split(jax.random.key(seed), 8)
    part_keys = jax.random.split(jax.random.fold_in(keys[7], part), 8)
    return {
        "feature_table": centred(part_keys[0], (NODES, D), 1.0, 6.0, ((0, 64), (1, 2)), jnp.float32),
        "own_features": centred(part_keys[1], (TARGETS, D), 1.0, 6.0, ((0, 64), (1, 2)), jnp.float32),
        "neighbor_ids": draw_neighbor_ids(jax.random.fold_in(jax.random.fold_in(keys[7], part), 71), part),
        "importance": jnp.clip(jnp.exp(math.log(5.0) - 2.3025851 * jax.random.uniform(part_keys[3], (TARGETS, NEIGH), jnp.float32) ** levels(part_keys[3], (TARGETS, NEIGH), ((0, 64),), -0.2, 0.2)), 0.5, 5.0),
        "w_self": centred(keys[4], (D, D), D ** -0.5, 0.1875, ((0, 2),)),
        "w_pool": centred(keys[5], (D, D), D ** -0.5, 0.1875, ((0, 2),)),
        "bias": draw_bias(jax.random.fold_in(keys[7], 71), part),
    }


def reference(feature_table, own_features, neighbor_ids, importance, w_self, w_pool, bias):
    weights = importance / lax.optimization_barrier(jnp.sum(importance, axis=1, keepdims=True))
    blocks = TARGETS // TGT_DEV

    def pool_block(operands):
        id_block, share_block = operands
        gathered = jnp.take(feature_table, id_block, axis=0)
        return lax.optimization_barrier(jnp.sum(share_block[:, :, None] * gathered, axis=1))
    pooled = lax.map(pool_block, (neighbor_ids.reshape(blocks, TGT_DEV, NEIGH), weights.reshape(blocks, TGT_DEV, NEIGH)))
    pooled = pooled.reshape(TARGETS, D)
    own_round = own_features.astype(jnp.bfloat16)
    pooled_round = pooled.astype(jnp.bfloat16)
    preact = jnp.dot(own_round, w_self, preferred_element_type=jnp.float32) + jnp.dot(pooled_round, w_pool, preferred_element_type=jnp.float32) + bias
    hidden = jnp.maximum(preact, 0.0)
    return hidden * lax.rsqrt(lax.optimization_barrier(jnp.mean(hidden * hidden, axis=1, keepdims=True)) + 1e-06)
```

```python
import functools
import math

import jax
import jax.numpy as jnp
from jax import lax
from jax.experimental import pallas as pl
from jax.experimental.pallas import tpu as pltpu
from jax.sharding import PartitionSpec as P

MESH = pl.DeviceIdType.MESH
NEIGH = 50
TGT = 16
CAP = 20
LANES = 128
F32 = jnp.float32
BF16 = jnp.bfloat16


def kernel(
    n,
    rows_dev,
    table_hbm,
    own_hbm,
    ids_hbm,
    imp_hbm,
    wself_hbm,
    wpool_hbm,
    bias_hbm,
    out_ref,
    tab,
    own_v,
    ids_v,
    imp_v,
    wself_v,
    wpool_v,
    bias_v,
    onehot,
    prefix,
    msg,
    got1,
    mid,
    got2,
    slots_v,
    slots_s,
    tgt_of,
    share_of,
    rows_g,
    self_part,
    rs_out,
    rs_in,
    fin,
    p2_in,
    ex_out,
    ex_in,
    in_sem,
    slot_sem,
    a1_send,
    a1_recv,
    a2_send,
    a2_recv,
    rs_send,
    rs_recv,
    p2_send,
    p2_recv,
    ex_sem,
):
    me = lax.axis_index("rows")
    col = lax.axis_index("cols")
    x = lax.rem(me, n)
    y = lax.div(me, n)
    owners = n * n
    half = n // 2
    width = own_v.shape[1]
    pieces = width // LANES
    tq = pieces // 2
    per_dev = own_v.shape[0]
    blocks = per_dev // TGT
    ring = lambda v: lax.rem(v + 2 * n, n)

    def along_x(k):
        return {"rows": y * n + ring(x + k)}

    def along_y(k):
        return {"rows": ring(y + k) * n + x}

    loads = [
        pltpu.make_async_copy(ids_hbm, ids_v, in_sem.at[0]),
        pltpu.make_async_copy(imp_hbm, imp_v, in_sem.at[1]),
        pltpu.make_async_copy(own_hbm, own_v, in_sem.at[2]),
        pltpu.make_async_copy(wself_hbm, wself_v, in_sem.at[3]),
        pltpu.make_async_copy(wpool_hbm, wpool_v, in_sem.at[4]),
        pltpu.make_async_copy(bias_hbm, bias_v, in_sem.at[5]),
    ]
    tab4 = tab.reshape(rows_dev // 8, pieces, 8, LANES)
    table_loads = [
        pltpu.make_async_copy(
            table_hbm.at[:, :, pl.ds(c * LANES, LANES)], tab4.at[:, c], in_sem.at[6 + c]
        )
        for c in range(pieces)
    ]
    for cp in loads[:2] + table_loads + loads[2:]:
        cp.start()

    barrier = pltpu.get_barrier_semaphore()
    for k in range(1, n):
        pl.semaphore_signal(barrier, inc=1, device_id=along_x(k), device_id_type=MESH)
        pl.semaphore_signal(barrier, inc=1, device_id=along_y(k), device_id_type=MESH)
    sibling = {"cols": 1 - col}
    pl.semaphore_signal(barrier, inc=1, device_id=sibling, device_id_type=MESH)

    loads[0].wait()
    loads[1].wait()
    lane = lax.broadcasted_iota(jnp.int32, (1, LANES), 1)
    owner_row = lax.broadcasted_iota(jnp.int32, (owners, LANES), 0)
    ids = ids_v[...]
    owner = ids >> int(math.log2(rows_dev))
    owner = jnp.where(ids < 0, -1, (owner & (n - 1)) * n + (owner >> int(math.log2(n))))
    for p in range(TGT):
        onehot[p * owners : (p + 1) * owners, :] = jnp.where(
            owner[p : p + 1] == owner_row, 1.0, 0.0
        ).astype(BF16)
    li = lax.broadcasted_iota(jnp.int32, (LANES, 2 * LANES), 0)
    lj = lax.broadcasted_iota(jnp.int32, (LANES, 2 * LANES), 1)
    hl = LANES // 2
    same = ((li // hl) == ((lj & (LANES - 1)) // hl)) & ((li < lj) | (lj >= LANES))
    prefix[...] = jnp.dot(
        onehot[...], jnp.where(same, 1.0, 0.0).astype(BF16), preferred_element_type=F32
    )
    imp = imp_v[...]
    left = jnp.sum(jnp.where(lane < hl, imp, 0.0), axis=1, keepdims=True)
    right = jnp.sum(jnp.where(lane >= hl, imp, 0.0), axis=1, keepdims=True)
    share = imp / jnp.where(lane < hl, left, right)
    local = ids & (rows_dev - 1)
    low = (local & 255).astype(F32)
    trow = lax.broadcasted_iota(jnp.int32, (TGT, LANES), 0)
    high = ((local >> 8) + trow * (rows_dev // 256)).astype(F32)
    share_hi = share.astype(BF16).astype(F32)
    share_lo = share - share_hi
    si = lax.broadcasted_iota(jnp.int32, (LANES, LANES), 0)
    sj = lax.broadcasted_iota(jnp.int32, (LANES, LANES), 1)
    slot_id = jnp.where(((si >> 5) & 1) == (sj // hl), si & 31, -1).astype(F32)
    base = jnp.zeros((owners, LANES), F32)
    acc = jnp.zeros((4 * owners, LANES), F32)
    for p in range(0, TGT, 2):
        lhs = []
        rhs = []
        for q in (p, p + 1):
            hot = onehot[q * owners : (q + 1) * owners, :].astype(F32)
            rank = jnp.sum(
                hot * (prefix[q * owners : (q + 1) * owners, :LANES] + base), axis=0, keepdims=True
            )
            base = base + prefix[q * owners : (q + 1) * owners, LANES:]
            rhs.append(jnp.where(slot_id == rank, 1.0, 0.0).astype(BF16))
            lhs.append(
                jnp.concatenate(
                    [hot * v[q : q + 1] for v in (low, high, share_hi, share_lo)], axis=0
                ).astype(BF16)
            )
        acc = acc + lax.dot_general(
            jnp.concatenate(lhs, axis=1),
            jnp.concatenate(rhs, axis=1),
            (((1,), (1,)), ((), ())),
            preferred_element_type=F32,
        )
    msg[0] = acc[:owners] + 256.0 * acc[owners : 2 * owners]
    msg[1] = acc[2 * owners : 3 * owners] + acc[3 * owners :]

    pad = jnp.zeros(((32 - CAP) * pieces, LANES), F32)

    def clear(i, carry):
        rows_g[pl.ds((i * 32 + CAP) * pieces, (32 - CAP) * pieces), :] = pad
        return carry

    lax.fori_loop(0, owners * blocks, clear, 0)

    pl.semaphore_wait(barrier, 2 * (n - 1) + 1)

    def hop1(k):
        to = ring(x + k)
        return pltpu.make_async_remote_copy(
            src_ref=msg.at[:, pl.ds(pl.multiple_of(to * n, n), n), :],
            dst_ref=got1.at[:, pl.ds(pl.multiple_of(x * n, n), n), :],
            send_sem=a1_send.at[k],
            recv_sem=a1_recv.at[k],
            device_id=along_x(k),
            device_id_type=MESH,
        )

    def hop2(k):
        return pltpu.make_async_remote_copy(
            src_ref=mid.at[ring(y + k)],
            dst_ref=got2.at[y],
            send_sem=a2_send.at[k],
            recv_sem=a2_recv.at[k],
            device_id=along_y(k),
            device_id_type=MESH,
        )

    order = sorted(range(1, n), key=lambda k: -min(k, n - k))
    for k in order:
        hop1(k).start()
    mine = pl.ds(pl.multiple_of(x * n, n), n)
    got1[:, mine, :] = msg[:, mine, :]

    loads[2].wait()
    loads[3].wait()
    self_part[...] = jnp.dot(own_v[...].astype(BF16), wself_v[...], preferred_element_type=F32)

    for k in order:
        hop1(k).wait_recv()
    for to in range(n):
        for plane in range(2):
            mid[to, plane * n : (plane + 1) * n, :] = got1[plane, pl.ds(to, n, stride=n), :]
    for k in order:
        hop2(k).start()
    got2[y] = mid[y]
    for cp in table_loads:
        cp.wait()
    for k in order:
        hop2(k).wait_recv()

    for s in range(n):
        packed = got2[s, :n, :].astype(jnp.int32)
        row = packed & (rows_dev - 1)
        slots_v[s * n : (s + 1) * n, :] = (row >> 3) * (8 * pieces) + (row & 7)
        tgt_of[s * n : (s + 1) * n, :] = (
            (packed >> int(math.log2(rows_dev))) + TGT * ((lane >> 5) & 1)
        ).astype(F32)
        share_of[s * n : (s + 1) * n, :] = got2[s, n:, :]
    to_scalar = pltpu.make_async_copy(slots_v, slots_s, slot_sem)
    to_scalar.start()
    to_scalar.wait()

    def gather(d, carry):
        for b in range(blocks):
            for s in range(CAP):
                start = slots_s[d, b * 32 + s]
                k = d * (32 * blocks) + b * 32 + s
                rows_g[pl.ds(k * pieces, pieces), :] = tab[pl.ds(start, pieces, stride=8), :]
        return carry

    lax.fori_loop(0, owners, gather, 0)

    group = 32 * blocks
    m = half * per_dev
    mi = lax.broadcasted_iota(jnp.int32, (m, LANES), 0).astype(F32)

    def partial(side, dest, sub):
        devs = [
            (sub * half + i) * n + dest if side == 0 else dest * n + sub * half + i
            for i in range(half)
        ]
        vals = jnp.concatenate(
            [
                jnp.concatenate(
                    [
                        rows_g[
                            pl.ds(d * (group * pieces) + side * tq + c, group, stride=pieces), :
                        ].astype(BF16)
                        for c in range(tq)
                    ],
                    axis=1,
                )
                for d in devs
            ],
            axis=0,
        )
        pick = []
        for j in range(0, half, 2):
            t = jnp.where(
                lane < hl,
                tgt_of[pl.ds(devs[j], 1), :] + float(j * per_dev),
                tgt_of[pl.ds(devs[j + 1], 1), :] + float((j + 1) * per_dev),
            )
            w = jnp.where(lane < hl, share_of[pl.ds(devs[j], 1), :], share_of[pl.ds(devs[j + 1], 1), :])
            pick.append(jnp.where(mi == t, w, 0.0).astype(BF16))
        return jnp.dot(jnp.concatenate(pick, axis=1), vals, preferred_element_type=F32)

    def hop(side, way, stage, sub):
        k = 1 if way == 0 else -1
        return pltpu.make_async_remote_copy(
            src_ref=rs_out.at[side, way, stage, sub],
            dst_ref=rs_in.at[side, way, stage, sub],
            send_sem=rs_send.at[side, way, stage, sub],
            recv_sem=rs_recv.at[side, way, stage, sub],
            device_id=along_x(k) if side == 0 else along_y(k),
            device_id_type=MESH,
        )

    def dest_of(side, way, stage):
        k = half - stage
        here = x if side == 0 else y
        return ring(here + k) if way == 0 else ring(here - k)

    for side in range(2):
        for way in range(2):
            rs_out[side, way, 0, way] = partial(side, dest_of(side, way, 0), way).astype(BF16)
            hop(side, way, 0, way).start()
    for side in range(2):
        for way in range(2):
            sub = 1 - way
            rs_out[side, way, 1, sub] = partial(side, dest_of(side, way, 1), sub).astype(BF16)
            hop(side, way, 1, sub).start()

    def stage_step(side, way, stage, sub):
        own = partial(side, dest_of(side, way, stage), sub)
        hop(side, way, stage - 1, sub).wait_recv()
        rs_out[side, way, stage, sub] = (
            own + rs_in[side, way, stage - 1, sub].astype(F32)
        ).astype(BF16)
        hop(side, way, stage, sub).start()

    for side in range(2):
        for way in range(2):
            stage_step(side, way, 1, way)

    def stages(stage, carry):
        for first in (1, 0):
            for side in range(2):
                for way in range(2):
                    stage_step(side, way, stage, way ^ first)
        return carry

    lax.fori_loop(2, half, stages, 0)

    def hop3(side, k):
        here = x if side == 1 else y
        return pltpu.make_async_remote_copy(
            src_ref=fin.at[side, ring(here + k)],
            dst_ref=p2_in.at[side, here],
            send_sem=p2_send.at[side, k],
            recv_sem=p2_recv.at[side, k],
            device_id=along_x(k) if side == 1 else along_y(k),
            device_id_type=MESH,
        )

    last = half - 1
    for side in range(2):
        for sub in range(2):
            total = partial(side, x if side == 0 else y, sub)
            for way in range(2):
                hop(side, way, last, sub).wait_recv()
                total = total + rs_in[side, way, last, sub].astype(F32)
            for i in range(half):
                fin[side, sub * half + i] = total[i * per_dev : (i + 1) * per_dev].astype(BF16)
        for k in order:
            hop3(side, k).start()

    sums = []
    for side in range(2):
        here = x if side == 1 else y
        total = fin[side, here].astype(F32)
        for k in order:
            hop3(side, k).wait_recv()
            total = total + p2_in[side, ring(here - k)].astype(F32)
        sums.append(total)
    pooled = jnp.concatenate(sums, axis=1).astype(BF16)
    loads[4].wait()
    loads[5].wait()
    ex_out[...] = self_part[...] + jnp.dot(pooled, wpool_v[...], preferred_element_type=F32)
    swap = pltpu.make_async_remote_copy(
        src_ref=ex_out,
        dst_ref=ex_in,
        send_sem=ex_sem.at[0],
        recv_sem=ex_sem.at[1],
        device_id=sibling,
        device_id_type=MESH,
    )
    swap.start()
    swap.wait_recv()
    hidden = jnp.maximum(ex_out[...] + ex_in[...] + bias_v[...], 0.0)
    scale = lax.rsqrt(jnp.sum(hidden * hidden, axis=1, keepdims=True) / hidden.shape[1] + 1e-6)
    columns = pl.ds(pl.multiple_of(col * width, width), width)
    mine_hidden = jnp.maximum(ex_out[:, columns] + ex_in[:, columns] + bias_v[:, columns], 0.0)
    out_ref[...] = mine_hidden * scale

    swap.wait_send()
    for k in range(1, n):
        hop1(k).wait_send()
        hop2(k).wait_send()
        for side in range(2):
            hop3(side, k).wait_send()
    for side in range(2):
        for way in range(2):
            hop(side, way, 0, way).wait_send()
            for stage in range(1, half):
                for sub in range(2):
                    hop(side, way, stage, sub).wait_send()


def body(feature_table, own_features, neighbor_ids, importance, w_self, w_pool, bias):
    rows_dev, width = feature_table.shape
    per_dev = own_features.shape[0]
    blocks = per_dev // TGT
    full = w_self.shape[1]
    n = math.isqrt(lax.axis_size("rows"))
    owners = n * n
    half = n // 2
    pieces = width // LANES
    slots = 32 * blocks
    lay = lambda a, fill: jnp.concatenate(
        [
            jnp.pad(part, ((0, 0), (0, LANES // 2 - NEIGH)), constant_values=fill)
            for part in (a[:TGT], a[TGT:])
        ],
        axis=1,
    )
    anyspace = pl.BlockSpec(memory_space=pl.ANY)
    dma = pltpu.SemaphoreType.DMA
    sub_rows = half * per_dev
    return pl.pallas_call(
        functools.partial(kernel, n, rows_dev),
        out_shape=jax.ShapeDtypeStruct((per_dev, width), F32),
        in_specs=[anyspace] * 7,
        out_specs=pl.BlockSpec(memory_space=pltpu.VMEM),
        scratch_shapes=[
            pltpu.VMEM((rows_dev * pieces, LANES), F32),
            pltpu.VMEM((per_dev, width), F32),
            pltpu.VMEM((TGT, LANES), jnp.int32),
            pltpu.VMEM((TGT, LANES), F32),
            pltpu.VMEM((width, full), BF16),
            pltpu.VMEM((width, full), BF16),
            pltpu.VMEM((1, full), F32),
            pltpu.VMEM((TGT * owners, LANES), BF16),
            pltpu.VMEM((TGT * owners, 2 * LANES), F32),
            pltpu.VMEM((2, owners, LANES), F32),
            pltpu.VMEM((2, owners, LANES), F32),
            pltpu.VMEM((n, 2 * n, LANES), F32),
            pltpu.VMEM((n, 2 * n, LANES), F32),
            pltpu.VMEM((owners, LANES), jnp.int32),
            pltpu.SMEM((owners, LANES), jnp.int32),
            pltpu.VMEM((owners, LANES), F32),
            pltpu.VMEM((owners, LANES), F32),
            pltpu.VMEM((owners * slots * pieces, LANES), F32),
            pltpu.VMEM((per_dev, full), F32),
            pltpu.VMEM((2, 2, half, 2, sub_rows, width // 2), BF16),
            pltpu.VMEM((2, 2, half, 2, sub_rows, width // 2), BF16),
            pltpu.VMEM((2, n, per_dev, width // 2), BF16),
            pltpu.VMEM((2, n, per_dev, width // 2), BF16),
            pltpu.VMEM((per_dev, full), F32),
            pltpu.VMEM((per_dev, full), F32),
            dma((6 + pieces,)),
            dma,
            dma((n,)),
            dma((n,)),
            dma((n,)),
            dma((n,)),
            dma((2, 2, half, 2)),
            dma((2, 2, half, 2)),
            dma((2, n)),
            dma((2, n)),
            dma((2,)),
        ],
        compiler_params=pltpu.CompilerParams(
            collective_id=0, has_side_effects=True, vmem_limit_bytes=48 * 1024 * 1024
        ),
    )(
        feature_table.reshape(rows_dev // 8, 8, width),
        own_features,
        lay(neighbor_ids, -1),
        lay(importance, 0),
        w_self,
        w_pool,
        bias.reshape(1, full),
    )


def solution(mesh):
    placed = (
        P(("groups", "rows"), "cols"),
        P(("groups", "rows"), "cols"),
        P(("groups", "rows"), None),
        P(("groups", "rows"), None),
        P("cols", None),
        P("cols", None),
        P(),
    )
    return jax.shard_map(
        body, mesh=mesh, in_specs=placed, out_specs=P(("groups", "rows"), "cols"), check_vma=False
    )
```

```python
import functools
import math

import jax
import jax.numpy as jnp
from jax import lax
from jax.experimental import pallas as pl
from jax.experimental.pallas import tpu as pltpu
from jax.sharding import PartitionSpec as P

MESH = pl.DeviceIdType.MESH
NEIGH = 50
TGT = 16
CAP = 20
LANES = 128
F32 = jnp.float32
BF16 = jnp.bfloat16


def kernel(
    n,
    rows_dev,
    table_hbm,
    own_hbm,
    ids_hbm,
    imp_hbm,
    wself_hbm,
    wpool_hbm,
    bias_hbm,
    out_ref,
    tab,
    own_v,
    ids_v,
    imp_v,
    wself_v,
    wpool_v,
    bias_v,
    onehot,
    prefix,
    msg,
    got1,
    mid,
    got2,
    slots_v,
    slots_s,
    tgt_of,
    share_of,
    rows_g,
    self_part,
    own_sum,
    rs_out,
    rs_in,
    fin,
    p2_in,
    ex_out,
    ex_in,
    in_sem,
    slot_sem,
    a1_send,
    a1_recv,
    a2_send,
    a2_recv,
    rs_send,
    rs_recv,
    p2_send,
    p2_recv,
    ex_sem,
):
    me = lax.axis_index("rows")
    col = lax.axis_index("cols")
    x = lax.rem(me, n)
    y = lax.div(me, n)
    owners = n * n
    half = n // 2
    width = own_v.shape[1]
    pieces = width // LANES
    tq = pieces // 2
    per_dev = own_v.shape[0]
    blocks = per_dev // TGT
    ring = lambda v: lax.rem(v + 2 * n, n)

    def along_x(k):
        return {"rows": y * n + ring(x + k)}

    def along_y(k):
        return {"rows": ring(y + k) * n + x}

    loads = [
        pltpu.make_async_copy(ids_hbm, ids_v, in_sem.at[0]),
        pltpu.make_async_copy(imp_hbm, imp_v, in_sem.at[1]),
        pltpu.make_async_copy(own_hbm, own_v, in_sem.at[2]),
        pltpu.make_async_copy(wself_hbm, wself_v, in_sem.at[3]),
        pltpu.make_async_copy(wpool_hbm, wpool_v, in_sem.at[4]),
        pltpu.make_async_copy(bias_hbm, bias_v, in_sem.at[5]),
    ]
    tab4 = tab.reshape(rows_dev // 8, pieces, 8, LANES)
    table_loads = [
        pltpu.make_async_copy(
            table_hbm.at[:, :, pl.ds(c * LANES, LANES)], tab4.at[:, c], in_sem.at[6 + c]
        )
        for c in range(pieces)
    ]
    for cp in loads[:2] + table_loads + loads[2:]:
        cp.start()

    barrier = pltpu.get_barrier_semaphore()
    for k in range(1, n):
        pl.semaphore_signal(barrier, inc=1, device_id=along_x(k), device_id_type=MESH)
        pl.semaphore_signal(barrier, inc=1, device_id=along_y(k), device_id_type=MESH)
    sibling = {"cols": 1 - col}
    pl.semaphore_signal(barrier, inc=1, device_id=sibling, device_id_type=MESH)

    loads[0].wait()
    loads[1].wait()
    lane = lax.broadcasted_iota(jnp.int32, (1, LANES), 1)
    owner_row = lax.broadcasted_iota(jnp.int32, (owners, LANES), 0)
    hl = LANES // 2

    def lay(a):
        room = jnp.zeros((TGT, hl - NEIGH), a.dtype)
        return jnp.concatenate([a[:TGT], room, a[TGT:], room], axis=1)

    real = (lane & (hl - 1)) < NEIGH
    ids = lay(ids_v[...])
    owner = ids >> int(math.log2(rows_dev))
    owner = jnp.where(real, (owner & (n - 1)) * n + (owner >> int(math.log2(n))), -1)
    for p in range(TGT):
        onehot[p * owners : (p + 1) * owners, :] = jnp.where(
            owner[p : p + 1] == owner_row, 1.0, 0.0
        ).astype(BF16)
    li = lax.broadcasted_iota(jnp.int32, (LANES, 2 * LANES), 0)
    lj = lax.broadcasted_iota(jnp.int32, (LANES, 2 * LANES), 1)
    same = ((li // hl) == ((lj & (LANES - 1)) // hl)) & ((li < lj) | (lj >= LANES))
    prefix[...] = jnp.dot(
        onehot[...], jnp.where(same, 1.0, 0.0).astype(BF16), preferred_element_type=F32
    )
    imp = lay(imp_v[...])
    left = jnp.sum(jnp.where(lane < hl, imp, 0.0), axis=1, keepdims=True)
    right = jnp.sum(jnp.where(lane >= hl, imp, 0.0), axis=1, keepdims=True)
    share = imp / jnp.where(lane < hl, left, right)
    local = ids & (rows_dev - 1)
    low = (local & 255).astype(F32)
    trow = lax.broadcasted_iota(jnp.int32, (TGT, LANES), 0)
    high = ((local >> 8) + trow * (rows_dev // 256)).astype(F32)
    share_hi = share.astype(BF16).astype(F32)
    share_lo = share - share_hi
    si = lax.broadcasted_iota(jnp.int32, (LANES, LANES), 0)
    sj = lax.broadcasted_iota(jnp.int32, (LANES, LANES), 1)
    slot_id = jnp.where(((si >> 5) & 1) == (sj // hl), si & 31, -1).astype(F32)
    base = jnp.zeros((owners, LANES), F32)
    acc = jnp.zeros((4 * owners, LANES), F32)
    for p in range(0, TGT, 2):
        lhs = []
        rhs = []
        for q in (p, p + 1):
            hot = onehot[q * owners : (q + 1) * owners, :].astype(F32)
            rank = jnp.sum(
                hot * (prefix[q * owners : (q + 1) * owners, :LANES] + base), axis=0, keepdims=True
            )
            base = base + prefix[q * owners : (q + 1) * owners, LANES:]
            rhs.append(jnp.where(slot_id == rank, 1.0, 0.0).astype(BF16))
            lhs.append(
                jnp.concatenate(
                    [hot * v[q : q + 1] for v in (low, high, share_hi, share_lo)], axis=0
                ).astype(BF16)
            )
        acc = acc + lax.dot_general(
            jnp.concatenate(lhs, axis=1),
            jnp.concatenate(rhs, axis=1),
            (((1,), (1,)), ((), ())),
            preferred_element_type=F32,
        )
    msg[...] = jnp.where(
        lane < hl,
        acc[:owners] + 256.0 * acc[owners : 2 * owners],
        acc[2 * owners : 3 * owners] + acc[3 * owners :],
    )

    pl.semaphore_wait(barrier, 2 * (n - 1) + 1)

    def hop1(k):
        to = ring(x + k)
        return pltpu.make_async_remote_copy(
            src_ref=msg.at[pl.ds(pl.multiple_of(to * n, n), n), :],
            dst_ref=got1.at[pl.ds(pl.multiple_of(x * n, n), n), :],
            send_sem=a1_send.at[k],
            recv_sem=a1_recv.at[k],
            device_id=along_x(k),
            device_id_type=MESH,
        )

    def hop2(k):
        return pltpu.make_async_remote_copy(
            src_ref=mid.at[ring(y + k)],
            dst_ref=got2.at[y],
            send_sem=a2_send.at[k],
            recv_sem=a2_recv.at[k],
            device_id=along_y(k),
            device_id_type=MESH,
        )

    order = sorted(range(1, n), key=lambda k: -min(k, n - k))
    for k in order:
        hop1(k).start()
    mine = pl.ds(pl.multiple_of(x * n, n), n)
    got1[mine, :] = msg[mine, :]

    pad = jnp.zeros(((32 - CAP) * pieces, LANES), F32)

    def clear(i, carry):
        rows_g[pl.ds((i * 32 + CAP) * pieces, (32 - CAP) * pieces), :] = pad
        return carry

    lax.fori_loop(0, owners * blocks, clear, 0)

    loads[2].wait()
    loads[3].wait()
    self_part[...] = jnp.dot(own_v[...].astype(BF16), wself_v[...], preferred_element_type=F32)

    near = order[::-1]
    for k in near:
        hop1(k).wait_recv()
    for to in range(n):
        mid[to] = got1[pl.ds(to, n, stride=n), :]
    for k in order:
        hop2(k).start()
    got2[y] = mid[y]
    for cp in table_loads:
        cp.wait()

    def to_scalar(at):
        rows = pl.ds(pl.multiple_of(at * n, n), n)
        return pltpu.make_async_copy(
            slots_v.at[rows, :], slots_s.at[rows, :], slot_sem.at[at]
        )

    def unpack(at):
        rows = pl.ds(pl.multiple_of(at * n, n), n)
        got = got2[at]
        turned = pltpu.roll(got, hl, axis=1)
        packed = jnp.where(lane < hl, got, turned).astype(jnp.int32)
        row = packed & (rows_dev - 1)
        slots_v[rows, :] = (row >> 3) * (8 * pieces) + (row & 7)
        tgt_of[rows, :] = (
            (packed >> int(math.log2(rows_dev))) + TGT * ((lane >> 5) & 1)
        ).astype(F32)
        share_of[rows, :] = jnp.where(lane < hl, turned, got)
        to_scalar(at).start()

    def gather(at):
        to_scalar(at).wait()

        def one(i, carry):
            d = at * n + i
            for b in range(blocks):
                for s in range(CAP):
                    start = slots_s[d, b * 32 + s]
                    k = d * (32 * blocks) + b * 32 + s
                    rows_g[pl.ds(k * pieces, pieces), :] = tab[pl.ds(start, pieces, stride=8), :]
            return carry

        lax.fori_loop(0, n, one, 0)

    unpack(y)
    before = y
    for k in near:
        hop2(k).wait_recv()
        unpack(ring(y - k))
        gather(before)
        before = ring(y - k)
    gather(before)

    group = 32 * blocks
    m = half * per_dev
    mi = lax.broadcasted_iota(jnp.int32, (m, LANES), 0).astype(F32)

    def partial(side, dest, sub):
        devs = [
            (sub * half + i) * n + dest if side == 0 else dest * n + sub * half + i
            for i in range(half)
        ]
        vals = jnp.concatenate(
            [
                jnp.concatenate(
                    [
                        rows_g[
                            pl.ds(d * (group * pieces) + side * tq + c, group, stride=pieces), :
                        ].astype(BF16)
                        for c in range(tq)
                    ],
                    axis=1,
                )
                for d in devs
            ],
            axis=0,
        )
        pick = []
        for j in range(0, half, 2):
            t = jnp.where(
                lane < hl,
                tgt_of[pl.ds(devs[j], 1), :] + float(j * per_dev),
                tgt_of[pl.ds(devs[j + 1], 1), :] + float((j + 1) * per_dev),
            )
            w = jnp.where(lane < hl, share_of[pl.ds(devs[j], 1), :], share_of[pl.ds(devs[j + 1], 1), :])
            pick.append(jnp.where(mi == t, w, 0.0).astype(BF16))
        return jnp.dot(jnp.concatenate(pick, axis=1), vals, preferred_element_type=F32)

    def hop(side, way, stage, sub, part):
        k = 1 if way == 0 else -1
        at = (side, way, stage, sub, part)
        return pltpu.make_async_remote_copy(
            src_ref=rs_out.at[at],
            dst_ref=rs_in.at[at],
            send_sem=rs_send.at[at],
            recv_sem=rs_recv.at[at],
            device_id=along_x(k) if side == 0 else along_y(k),
            device_id_type=MESH,
        )

    def dest_of(side, way, stage):
        k = half - stage
        here = x if side == 0 else y
        return ring(here + k) if way == 0 else ring(here - k)

    lanes4 = [(side, way) for side in range(2) for way in range(2)]
    pm = m // 2

    def send_first(side, way, stage, sub):
        own = partial(side, dest_of(side, way, stage), sub)
        for part in range(2):
            rs_out[side, way, stage, sub, part] = own[part * pm : (part + 1) * pm].astype(BF16)
            hop(side, way, stage, sub, part).start()

    def ahead(side, way, stage, sub):
        own_sum[side, way, sub] = partial(side, dest_of(side, way, stage), sub)

    def pass_on(side, way, stage, sub, part):
        hop(side, way, stage - 1, sub, part).wait_recv()
        rs_out[side, way, stage, sub, part] = (
            own_sum[side, way, sub, pl.ds(part * pm, pm)]
            + rs_in[side, way, stage - 1, sub, part].astype(F32)
        ).astype(BF16)
        hop(side, way, stage, sub, part).start()

    for side, way in lanes4:
        send_first(side, way, 0, way)
    for side, way in lanes4:
        send_first(side, way, 1, 1 - way)
    last = half - 1
    for stage in range(1, half):
        for side, way in lanes4:
            ahead(side, way, stage, way)
        for part in range(2):
            for side, way in lanes4:
                pass_on(side, way, stage, way, part)
        if stage < last:
            for side, way in lanes4:
                ahead(side, way, stage + 1, 1 - way)
            for part in range(2):
                for side, way in lanes4:
                    pass_on(side, way, stage + 1, 1 - way, part)

    def hop3(side, to):
        here = x if side == 1 else y
        return pltpu.make_async_remote_copy(
            src_ref=fin.at[side, to],
            dst_ref=p2_in.at[side, here],
            send_sem=p2_send.at[side, to],
            recv_sem=p2_recv.at[side, here],
            device_id={"rows": y * n + to} if side == 1 else {"rows": to * n + x},
            device_id_type=MESH,
        )

    def hop3_from(side, k):
        here = x if side == 1 else y
        there = ring(here - k)
        return pltpu.make_async_remote_copy(
            src_ref=fin.at[side, there],
            dst_ref=p2_in.at[side, there],
            send_sem=p2_send.at[side, there],
            recv_sem=p2_recv.at[side, there],
            device_id=along_x(-k) if side == 1 else along_y(-k),
            device_id_type=MESH,
        )

    for side in range(2):
        for sub in range(2):
            own_sum[side, 0, sub] = partial(side, x if side == 0 else y, sub)
    per_part = half // 2
    for part in range(2):
        for side in range(2):
            for sub in range(2):
                total = own_sum[side, 0, sub, pl.ds(part * pm, pm)]
                for way in (1 - sub, sub):
                    hop(side, way, last, sub, part).wait_recv()
                    total = total + rs_in[side, way, last, sub, part].astype(F32)
                for i in range(per_part):
                    to = sub * half + part * per_part + i
                    fin[side, to] = total[i * per_dev : (i + 1) * per_dev].astype(BF16)

                    @pl.when(to != (x if side == 1 else y))
                    def _():
                        hop3(side, to).start()

    sums = []
    for side in range(2):
        here = x if side == 1 else y
        total = fin[side, here].astype(F32)
        for k in near:
            hop3_from(side, k).wait_recv()
            total = total + p2_in[side, ring(here - k)].astype(F32)
        sums.append(total)
    pooled = jnp.concatenate(sums, axis=1).astype(BF16)
    loads[4].wait()
    loads[5].wait()
    ex_out[...] = self_part[...] + jnp.dot(pooled, wpool_v[...], preferred_element_type=F32)
    swap = pltpu.make_async_remote_copy(
        src_ref=ex_out,
        dst_ref=ex_in,
        send_sem=ex_sem.at[0],
        recv_sem=ex_sem.at[1],
        device_id=sibling,
        device_id_type=MESH,
    )
    swap.start()
    for k in range(1, n):
        hop1(k).wait_send()
        hop2(k).wait_send()
        for side in range(2):
            hop3_from(side, k).wait_send()
    for side, way in lanes4:
        for part in range(2):
            hop(side, way, 0, way, part).wait_send()
            for stage in range(1, half):
                for sub in range(2):
                    hop(side, way, stage, sub, part).wait_send()
    swap.wait_recv()
    hidden = jnp.maximum(ex_out[...] + ex_in[...] + bias_v[...], 0.0)
    scale = lax.rsqrt(jnp.sum(hidden * hidden, axis=1, keepdims=True) / hidden.shape[1] + 1e-6)
    columns = pl.ds(pl.multiple_of(col * width, width), width)
    mine_hidden = jnp.maximum(ex_out[:, columns] + ex_in[:, columns] + bias_v[:, columns], 0.0)
    out_ref[...] = mine_hidden * scale

    swap.wait_send()


def body(feature_table, own_features, neighbor_ids, importance, w_self, w_pool, bias):
    rows_dev, width = feature_table.shape
    per_dev = own_features.shape[0]
    blocks = per_dev // TGT
    full = w_self.shape[1]
    n = math.isqrt(lax.axis_size("rows"))
    owners = n * n
    half = n // 2
    pieces = width // LANES
    slots = 32 * blocks
    in_hbm = pl.BlockSpec(memory_space=pltpu.HBM)
    dma = pltpu.SemaphoreType.DMA
    sub_rows = half * per_dev
    return pl.pallas_call(
        functools.partial(kernel, n, rows_dev),
        out_shape=jax.ShapeDtypeStruct((per_dev, width), F32),
        in_specs=[in_hbm] * 7,
        out_specs=pl.BlockSpec(memory_space=pltpu.VMEM),
        scratch_shapes=[
            pltpu.VMEM((rows_dev * pieces, LANES), F32),
            pltpu.VMEM((per_dev, width), F32),
            pltpu.VMEM((per_dev, NEIGH), jnp.int32),
            pltpu.VMEM((per_dev, NEIGH), F32),
            pltpu.VMEM((width, full), BF16),
            pltpu.VMEM((width, full), BF16),
            pltpu.VMEM((1, full), F32),
            pltpu.VMEM((TGT * owners, LANES), BF16),
            pltpu.VMEM((TGT * owners, 2 * LANES), F32),
            pltpu.VMEM((owners, LANES), F32),
            pltpu.VMEM((owners, LANES), F32),
            pltpu.VMEM((n, n, LANES), F32),
            pltpu.VMEM((n, n, LANES), F32),
            pltpu.VMEM((owners, LANES), jnp.int32),
            pltpu.SMEM((owners, LANES), jnp.int32),
            pltpu.VMEM((owners, LANES), F32),
            pltpu.VMEM((owners, LANES), F32),
            pltpu.VMEM((owners * slots * pieces, LANES), F32),
            pltpu.VMEM((per_dev, full), F32),
            pltpu.VMEM((2, 2, 2, sub_rows, width // 2), F32),
            pltpu.VMEM((2, 2, half, 2, 2, sub_rows // 2, width // 2), BF16),
            pltpu.VMEM((2, 2, half, 2, 2, sub_rows // 2, width // 2), BF16),
            pltpu.VMEM((2, n, per_dev, width // 2), BF16),
            pltpu.VMEM((2, n, per_dev, width // 2), BF16),
            pltpu.VMEM((per_dev, full), F32),
            pltpu.VMEM((per_dev, full), F32),
            dma((6 + pieces,)),
            dma((n,)),
            dma((n,)),
            dma((n,)),
            dma((n,)),
            dma((n,)),
            dma((2, 2, half, 2, 2)),
            dma((2, 2, half, 2, 2)),
            dma((2, n)),
            dma((2, n)),
            dma((2,)),
        ],
        compiler_params=pltpu.CompilerParams(
            collective_id=0, has_side_effects=True, vmem_limit_bytes=67043328
        ),
    )(
        feature_table.reshape(rows_dev // 8, 8, width),
        own_features,
        neighbor_ids,
        importance,
        w_self,
        w_pool,
        bias.reshape(1, full),
    )


def solution(mesh):
    placed = (
        P(("groups", "rows"), "cols"),
        P(("groups", "rows"), "cols"),
        P(("groups", "rows"), None),
        P(("groups", "rows"), None),
        P("cols", None),
        P("cols", None),
        P(),
    )
    return jax.shard_map(
        body, mesh=mesh, in_specs=placed, out_specs=P(("groups", "rows"), "cols"), check_vma=False
    )
```
